512 devices in a mesh: blk: 128 (over z, y, core), lblk: 4 (over x).
Axes of the slice: x: 4, y: 4, z: 16, core: 2. Of those that a mesh axis runs over, the one named last changes fastest.
Arguments:
- sky: bfloat16 [8, 2, 512, 16384], P(None, None, 'blk', 'lblk'), may hold values from -6 to 6
- arc_start: int32 [2, 512], P(None, 'blk'), may hold values from 0 to 16383
- arc_count: int32 [2, 512], P(None, 'blk'), may hold values from 4096 to 16384
- owner_modes: int32 [512], replicated, may hold values from 0 to 511, each once
- legendre: bfloat16 [512, 128, 4, 4096], P('blk', None, None, 'lblk'), may hold values from -0.25 to 0.25
Outputs:
- alm: float32 [8, 2, 512, 4096], P(None, None, 'blk', 'lblk')
The draws below stay inside these ranges and needn't reach their ends.
Inputs may be any that keep to these rules, and one draw needn't show every extreme that they name: `owner_modes`: each m-mode 0 to 511 appears exactly once.
All inputs are finite; a program needn't handle non-finite values.
Results may differ from the reference program's by a relative error of at most 0.0049.
Values may be sent and summed in bfloat16 or wider, within the bound.
A program may use at most 64 MiB of HBM per device.

```python
import math
import jax
import jax.numpy as jnp
from jax import lax

RLEN = 16384
L = 4096
CYCLE_DEV = 4
MAPS = 8
M_SLAB = 512
CYCLES_HALF = 512


def plant(result, stream_key, smallest, largest):
    extent = result.shape
    place = [jax.random.randint(jax.random.fold_in(stream_key, axis), (), 0, extent[axis]) for axis in range(len(extent))]
    result = result.at[tuple(place)].set(smallest)
    longest = extent.index(max(extent))
    place[longest] = (place[longest] + 1) % extent[longest]
    return result.at[tuple(place)].set(largest)


def steps_of(stream_key, dims, cuts, smallest, high):
    factor_of = 1.0
    for dim, blocks in cuts:
        heights = jax.random.uniform(jax.random.fold_in(jax.random.fold_in(stream_key, 6), dim), (blocks,), jnp.float32, smallest / len(cuts), high / len(cuts))
        factor_of = factor_of * jnp.repeat(jnp.exp(heights), dims[dim] // blocks).reshape((-1,) + (1,) * (len(dims) - 1 - dim))
    return factor_of


def normal_values(stream_key, extent, spread, bound, shards=(), kind=jnp.bfloat16):
    result = spread * jax.random.normal(stream_key, extent, jnp.float32)
    if shards:
        result = result * steps_of(stream_key, extent, shards, -0.22, 0.18)
    return jnp.clip(result, -bound, bound).astype(kind)


def setup_inputs(seed: int = 0) -> dict:
    key_list = jax.random.split(jax.random.key(seed), 6)
    return {
        "sky": normal_values(key_list[0], (MAPS, 2, CYCLES_HALF, RLEN), 1.0, 6.0, ((2, 128), (3, 4))),
        "arc_start": plant(jax.random.randint(key_list[1], (2, CYCLES_HALF), 0, RLEN), jax.random.fold_in(key_list[1], 1), 0, RLEN - 1).astype(jnp.int32),
        "arc_count": plant(jax.random.randint(key_list[2], (2, CYCLES_HALF), RLEN // 4, RLEN + 1), jax.random.fold_in(key_list[2], 1), RLEN // 4, RLEN).astype(jnp.int32),
        "owner_modes": jax.random.permutation(key_list[3], M_SLAB).astype(jnp.int32),
        "legendre": normal_values(key_list[4], (M_SLAB, CYCLES_HALF // CYCLE_DEV, CYCLE_DEV, L), CYCLES_HALF ** -0.5, 0.25, ((0, 128), (3, 4))),
    }


DIFFUSION = 0.2

def mode_basis(positions, mode_list):
    product_index = jnp.mod(positions[:, None] * mode_list[None, :], RLEN)
    angles = 2.0 * math.pi / RLEN * product_index.astype(jnp.float32)
    return (jnp.cos(angles).astype(jnp.bfloat16), (-jnp.sin(angles)).astype(jnp.bfloat16))

def smooth_map(one_map, arc_start, arc_count):
    pixels = jnp.arange(RLEN, dtype=jnp.int32)
    offset = jnp.mod(pixels[None, None, :] - arc_start[:, :, None], RLEN)
    kept_mask = offset < arc_count[:, :, None]
    centre = jnp.where(kept_mask, one_map, jnp.zeros((), one_map.dtype)).astype(jnp.float32)
    zero_row = jnp.zeros_like(centre[:, :1])
    layer_above = jnp.concatenate([zero_row, centre[:, :-1]], axis=1)
    layer_below = jnp.concatenate([centre[:, 1:], centre[::-1, -1:]], axis=1)
    pixel_before = jnp.roll(centre, 1, axis=2)
    pixel_after = jnp.roll(centre, -1, axis=2)
    total = layer_above + layer_below + pixel_before + pixel_after - 4.0 * centre
    return (centre + DIFFUSION * total).astype(jnp.bfloat16)

def reference(sky, arc_start, arc_count, owner_modes, legendre):
    pixels = jnp.arange(RLEN, dtype=jnp.int32)
    cos_table, sin_table = mode_basis(pixels, owner_modes)
    parity = jnp.arange(CYCLES_HALF, dtype=jnp.int32) % 2
    phase_turn = math.pi / RLEN * (parity[:, None] * owner_modes[None, :]).astype(jnp.float32)
    turn_cos = jnp.cos(phase_turn)
    turn_sin = jnp.sin(phase_turn)
    norm_scale = 1.0 / math.sqrt(RLEN)

    def fourier_map(one_map):
        smooth = smooth_map(one_map, arc_start, arc_count)
        flat_rows = smooth.reshape(-1, RLEN)
        real_part = jnp.dot(flat_rows, cos_table, preferred_element_type=jnp.float32).reshape(2, CYCLES_HALF, -1)
        imag_part = jnp.dot(flat_rows, sin_table, preferred_element_type=jnp.float32).reshape(2, CYCLES_HALF, -1)
        rotated_real = (real_part * turn_cos + imag_part * turn_sin) * norm_scale
        rotated_imag = (imag_part * turn_cos - real_part * turn_sin) * norm_scale
        return jnp.stack([rotated_real, rotated_imag], axis=2).astype(jnp.bfloat16)
    fourier = lax.map(fourier_map, sky)
    north_part = fourier[:, 0].astype(jnp.float32)
    south_part = fourier[:, 1].astype(jnp.float32)
    folded = jnp.concatenate([north_part + south_part, north_part - south_part], axis=2).astype(jnp.bfloat16)
    degrees = jnp.arange(L, dtype=jnp.int32)

    def mode_section(inputs):
        block, folded_mode, mode = inputs
        legendre_rows = block.reshape(-1, L).astype(jnp.float32)
        latitude_sums = jnp.einsum('xry,rl->xyl', folded_mode.astype(jnp.float32), legendre_rows, precision=lax.Precision.HIGHEST)
        even_parity = jnp.mod(degrees + mode, 2) == 0
        chosen = jnp.where(even_parity[None, None, :], latitude_sums[:, :2], latitude_sums[:, 2:])
        return jnp.where((degrees >= mode)[None, None, :], chosen, jnp.zeros((), jnp.float32))
    stacked = lax.map(mode_section, (legendre, jnp.moveaxis(folded, 3, 0), owner_modes))
    return jnp.transpose(stacked, (1, 2, 0, 3))
```

```python
import math

import jax
import jax.numpy as jnp
from jax import lax
from jax.experimental import pallas as pl
from jax.experimental.pallas import tpu as pltpu
from jax.sharding import PartitionSpec as P

RLEN = 16384
DIFFUSION = 0.2
NX = 4
NZ = 16
NYC = 8
NBLK = NZ * NYC
LANES = 128
G_STRIDE = 40
BF16 = jnp.bfloat16
F32 = jnp.float32


def unit_circle(t):
    t = t & (RLEN - 1)
    q = (t + 2048) >> 12
    theta = (t - (q << 12)).astype(F32) * (2.0 * math.pi / RLEN)
    u = theta * theta
    s = theta * (1.0 + u * (-1.0 / 6 + u * (1.0 / 120 + u * (-1.0 / 5040 + u * (1.0 / 362880)))))
    c = 1.0 + u * (-0.5 + u * (1.0 / 24 + u * (-1.0 / 720 + u * (1.0 / 40320))))
    odd = (q & 1) == 1
    big = jnp.where(odd, s, c)
    small = jnp.where(odd, c, s)
    cos = jnp.where(((q + 1) & 2) == 2, -big, big)
    sin = jnp.where((q & 2) == 2, -small, small)
    return cos, sin


def small_angle(theta):
    u = theta * theta
    s = theta * (1.0 + u * (-1.0 / 6 + u * (1.0 / 120 + u * (-1.0 / 5040))))
    c = 1.0 + u * (-0.5 + u * (1.0 / 24 + u * (-1.0 / 720 + u * (1.0 / 40320))))
    return c, s


def iota(shape, dim):
    return lax.broadcasted_iota(jnp.int32, shape, dim)


def kernel(
    sky_hbm,
    start_ref,
    count_ref,
    modes_s,
    modes_v,
    leg_hbm,
    out_ref,
    sky_v,
    x_ref,
    y_ref,
    modes_ref,
    rs_send,
    rs_recv,
    u_ref,
    z_send,
    z_recv,
    zf_ref,
    g_send,
    g_recv,
    gf_ref,
    leg_raw,
    leg_tmp,
    leg_prep,
    sky_sem,
    leg_sem,
    rs_ssem,
    rs_rsem,
    z_ssem,
    z_rsem,
    g_ssem,
    g_rsem,
):
    blk = lax.axis_index("blk")
    col = lax.axis_index("lblk")
    my_z = blk // NYC
    my_yc = blk % NYC

    sky_copy = pltpu.make_async_copy(sky_hbm, sky_v, sky_sem)
    sky_copy.start()
    leg_copy = pltpu.make_async_copy(leg_hbm, leg_raw, leg_sem)
    leg_copy.start()

    barrier = pltpu.get_barrier_semaphore()

    def greet_z(d, carry):
        pl.semaphore_signal(
            barrier,
            inc=1,
            device_id={"blk": ((my_z + d) % NZ) * NYC + my_yc, "lblk": col},
            device_id_type=pl.DeviceIdType.MESH,
        )
        return carry

    def greet_yx(d, carry):
        pl.semaphore_signal(
            barrier,
            inc=1,
            device_id={
                "blk": my_z * NYC + (my_yc + d // NX) % NYC,
                "lblk": (col + d % NX) % NX,
            },
            device_id_type=pl.DeviceIdType.MESH,
        )
        return carry

    lax.fori_loop(1, NZ, greet_z, 0)
    lax.fori_loop(1, NYC * NX, greet_yx, 0)

    lane8 = iota((8, LANES), 1)
    pick = (4 * (lane8 & 31) + iota((8, LANES), 0)) & (LANES - 1)
    modes = jnp.zeros((8, LANES), jnp.int32)
    for r in range(4):
        row = jnp.broadcast_to(modes_v[r : r + 1, :], (8, LANES))
        got = jnp.take_along_axis(row, pick, axis=1)
        modes = jnp.where((lane8 >> 5) == r, got, modes)
    modes_ref[...] = modes

    sky_copy.wait()
    sub8 = iota((8, LANES), 0)
    k8 = sub8 & 3
    for h in range(2):
        start8 = jnp.zeros((8, LANES), jnp.int32)
        count8 = jnp.zeros((8, LANES), jnp.int32)
        for k in range(4):
            start8 = jnp.where(k8 == k, start_ref[h, k], start8)
            count8 = jnp.where(k8 == k, count_ref[h, k], count8)
        base8 = col * 4096 + (sub8 >> 2) * LANES + lane8 - start8
        keep = [
            ((base8 + 256 * t) & (RLEN - 1)) < count8 for t in range(16)
        ]
        keep = [jnp.where(b, 1.0, 0.0).astype(F32) for b in keep]
        keep_lo = jnp.concatenate(keep[:8], axis=0)
        keep_hi = jnp.concatenate(keep[8:], axis=0)
        for x in range(8):
            r0 = (x * 2 + h) * 128
            lo = sky_v[pl.ds(r0, 64), :].astype(F32)
            hi = sky_v[pl.ds(r0 + 64, 64), :].astype(F32)
            x_ref[pl.ds((x * 2 + h) * 64, 64), 0:128] = (lo * keep_lo).astype(BF16)
            x_ref[pl.ds((x * 2 + h) * 64, 64), 128:256] = (hi * keep_hi).astype(BF16)

    upper = sub8 < 4
    for step, ahead in enumerate((2, 1, 3, 0)):
        chunk = (col + ahead) % NX
        m_row = modes_ref[pl.ds(chunk, 1), :]
        b_index = iota((LANES, LANES), 0)
        lo_c, lo_s = unit_circle(b_index * m_row)
        hi_c, hi_s = unit_circle((b_index + 2048) * m_row)
        table = jnp.concatenate(
            [
                jnp.concatenate([lo_c, -lo_s], axis=1),
                jnp.concatenate([hi_c, -hi_s], axis=1),
            ],
            axis=0,
        ).astype(BF16)
        y_ref[...] = jnp.dot(x_ref[...], table, preferred_element_type=F32)
        lt_index = iota((64, LANES), 0) >> 2
        w_c, w_s = unit_circle((col * 4096 + lt_index * LANES) * m_row)
        w_c = w_c * (1.0 / 128)
        w_s = w_s * (-1.0 / 128)
        for x in range(8):
            acc = []
            for h in range(2):
                re = jnp.zeros((8, LANES), F32)
                im = jnp.zeros((8, LANES), F32)
                for t in range(8):
                    r0 = (x * 2 + h) * 64 + t * 8
                    yc = y_ref[r0 : r0 + 8, 0:128]
                    ys = y_ref[r0 : r0 + 8, 128:256]
                    wc = w_c[t * 8 : t * 8 + 8]
                    ws = w_s[t * 8 : t * 8 + 8]
                    re = re + (yc * wc - ys * ws)
                    im = im + (yc * ws + ys * wc)
                acc.append((re, im))
            for part in range(2):
                plus = acc[0][part] + acc[1][part]
                minus = acc[0][part] - acc[1][part]
                plus = plus + pltpu.roll(plus, 4, axis=0)
                minus = minus + pltpu.roll(minus, 4, axis=0)
                r0 = part * 64 + x * 8
                u_ref[r0 : r0 + 8, :] = jnp.where(upper, plus, minus)
        if ahead == 0:
            break
        rs_send[step] = u_ref[...].astype(BF16)
        if step == 0:
            pl.semaphore_wait(barrier, NZ - 1 + NYC * NX - 1)
        pltpu.make_async_remote_copy(
            src_ref=rs_send.at[step],
            dst_ref=rs_recv.at[step],
            send_sem=rs_ssem.at[step],
            recv_sem=rs_rsem.at[step],
            device_id={"blk": blk, "lblk": chunk},
            device_id_type=pl.DeviceIdType.MESH,
        ).start()

    def prepare(s):
        def group(gb, carry):
            raw = leg_raw[s, pl.ds(gb * 512, 512), :].astype(F32)
            for g in range(16):
                leg_tmp[g * G_STRIDE : g * G_STRIDE + 32, :] = raw[g * 32 : g * 32 + 32]
            for lt in range(8):
                for r in range(4):
                    rows = leg_tmp[pl.ds(lt * 4 + r, 16, stride=G_STRIDE), :]
                    leg_prep[s, pl.ds(r * 128 + gb * 16, 16), lt * 128 : lt * 128 + 128] = (
                        rows.astype(BF16)
                    )
            return carry

        lax.fori_loop(0, 8, group, 0)

    leg_copy.wait()
    prepare(0)

    def rs_copy(step):
        return pltpu.make_async_remote_copy(
            src_ref=rs_send.at[step],
            dst_ref=rs_recv.at[step],
            send_sem=rs_ssem.at[step],
            recv_sem=rs_rsem.at[step],
            device_id={"blk": blk, "lblk": (col + 1) % NX},
            device_id_type=pl.DeviceIdType.MESH,
        )

    total = u_ref[...]
    for step in range(3):
        rs_copy(step).wait_recv()
    for step in range(3):
        total = total + rs_recv[step].astype(F32)
    u_ref[...] = total

    ordered = jnp.concatenate(
        [
            u_ref[pl.ds(part * 64 + sign * 4 + k, 8, stride=8), :]
            for k in range(4)
            for part in range(2)
            for sign in range(2)
        ],
        axis=0,
    )
    turned = ordered.T
    for z in range(NZ):
        z_send[z] = turned[z * 8 : z * 8 + 8].astype(BF16)

    def z_copy(d):
        return pltpu.make_async_remote_copy(
            src_ref=z_send.at[(my_z + d) % NZ],
            dst_ref=z_recv.at[my_z],
            send_sem=z_ssem.at[d],
            recv_sem=z_rsem.at[d],
            device_id={"blk": ((my_z + d) % NZ) * NYC + my_yc, "lblk": col},
            device_id_type=pl.DeviceIdType.MESH,
        )

    for d in (8, 7, 9, 6, 10, 5, 11, 4, 12, 3, 13, 2, 14, 1, 15):
        z_copy(d).start()
    z_recv[my_z] = z_send[my_z]
    prepare(1)
    prepare(2)
    prepare(3)

    def z_wait(d, carry):
        z_copy(d).wait_recv()
        return carry

    lax.fori_loop(1, NZ, z_wait, 0)
    for z in range(NZ):
        zf_ref[z * 8 : z * 8 + 8, :] = z_recv[z].astype(F32)
    for yc in range(NYC):
        g_send[yc] = zf_ref[pl.ds(yc, NZ, stride=8), :].astype(BF16)

    def g_copy(d):
        yc = (my_yc + d // NX) % NYC
        return pltpu.make_async_remote_copy(
            src_ref=g_send.at[yc],
            dst_ref=g_recv.at[col, my_yc],
            send_sem=g_ssem.at[d],
            recv_sem=g_rsem.at[d],
            device_id={"blk": my_z * NYC + yc, "lblk": (col + d % NX) % NX},
            device_id_type=pl.DeviceIdType.MESH,
        )

    for dx in (0, 2, 1, 3):
        for dyc in (4, 5, 3, 2, 6, 7, 1, 0):
            if dx or dyc:
                g_copy(dyc * NX + dx).start()
    g_recv[col, my_yc] = g_send[my_yc]

    lane_row = iota((8, LANES), 1)
    degree = iota((8, 1024), 1) + col * 1024
    for ahead in (0, 1, 3, 2):
        source = (col + NX - ahead) % NX

        def g_wait(j, carry, ahead=ahead):
            g_copy(j * NX + ahead).wait_recv()
            return carry

        lax.fori_loop(1 if ahead == 0 else 0, NYC, g_wait, 0)
        for yc in range(NYC):
            gf_ref[yc * NZ : yc * NZ + NZ, :] = g_recv[source, yc].astype(F32)
        by_cycle = jnp.concatenate(
            [gf_ref[pl.ds(z, NYC, stride=NZ), :] for z in range(NZ)], axis=0
        )
        turned = by_cycle.T
        mode = modes_s[blk * NX + source]
        theta = jnp.full((8, LANES), mode, jnp.int32).astype(F32) * (math.pi / RLEN)
        turn_c, turn_s = small_angle(theta)
        double_c, _ = small_angle(theta * 2.0)
        centre = (1.0 - 4.0 * DIFFUSION) + 2.0 * DIFFUSION * double_c
        rows = {}
        for sign in range(2):
            smooth = {}
            for part in range(2):
                a = [
                    turned[(k * 4 + part * 2 + sign) * 8 : (k * 4 + part * 2 + sign) * 8 + 8]
                    for k in range(4)
                ]
                above = jnp.where(lane_row == 0, 0.0, pltpu.roll(a[3], 1, axis=1))
                edge = a[3] if sign == 0 else -a[3]
                below = jnp.where(
                    lane_row == LANES - 1, edge, pltpu.roll(a[0], LANES - 1, axis=1)
                )
                full = [above] + a + [below]
                for k in range(4):
                    smooth[part, k] = centre * a[k] + DIFFUSION * (full[k] + full[k + 2])
            for k in range(4):
                re, im = smooth[0, k], smooth[1, k]
                if k % 2:
                    re, im = re * turn_c + im * turn_s, im * turn_c - re * turn_s
                rows[sign, 0, k] = re
                rows[sign, 1, k] = im
        lhs = jnp.concatenate(
            [
                jnp.concatenate(
                    [rows[sign, part, k] for sign in range(2) for part in range(2)], axis=0
                )
                for k in range(4)
            ],
            axis=1,
        ).astype(BF16)
        sums = jnp.dot(lhs, leg_prep[source], preferred_element_type=F32)
        even = ((degree + mode) & 1) == 0
        inside = degree >= mode
        for part in range(2):
            chosen = jnp.where(
                even, sums[part * 8 : part * 8 + 8], sums[16 + part * 8 : 24 + part * 8]
            )
            chosen = jnp.where(inside, chosen, 0.0)
            for lt in range(8):
                out_ref[pl.ds(part * 32 + lt * 4 + source, 8, stride=64), :] = chosen[
                    :, lt * 128 : lt * 128 + 128
                ]

    for step in range(3):
        rs_copy(step).wait_send()

    def z_done(d, carry):
        z_copy(d).wait_send()
        return carry

    def g_done(d, carry):
        g_copy(d).wait_send()
        return carry

    lax.fori_loop(1, NZ, z_done, 0)
    lax.fori_loop(1, NYC * NX, g_done, 0)


def local(sky, arc_start, arc_count, owner_modes, legendre):
    sky_rows = sky.reshape(16, 4, 32, 128).transpose(0, 2, 1, 3).reshape(2048, 128)
    leg_rows = (
        legendre.reshape(4, 128, 4, 8, 128).transpose(0, 1, 3, 2, 4).reshape(4, 4096, 128)
    )
    any_space = pl.BlockSpec(memory_space=pl.ANY)
    vmem = pl.BlockSpec(memory_space=pltpu.VMEM)
    smem = pl.BlockSpec(memory_space=pltpu.SMEM)
    out = pl.pallas_call(
        kernel,
        out_shape=jax.ShapeDtypeStruct((512, 128), F32),
        in_specs=[any_space, smem, smem, smem, vmem, any_space],
        out_specs=vmem,
        scratch_shapes=[
            pltpu.VMEM((2048, 128), BF16),
            pltpu.VMEM((1024, 256), BF16),
            pltpu.VMEM((1024, 256), F32),
            pltpu.VMEM((8, 128), jnp.int32),
            pltpu.VMEM((3, 128, 128), BF16),
            pltpu.VMEM((3, 128, 128), BF16),
            pltpu.VMEM((128, 128), F32),
            pltpu.VMEM((NZ, 8, 128), BF16),
            pltpu.VMEM((NZ, 8, 128), BF16),
            pltpu.VMEM((128, 128), F32),
            pltpu.VMEM((NYC, NZ, 128), BF16),
            pltpu.VMEM((NX, NYC, NZ, 128), BF16),
            pltpu.VMEM((128, 128), F32),
            pltpu.VMEM((4, 4096, 128), BF16),
            pltpu.VMEM((16 * G_STRIDE, 128), F32),
            pltpu.VMEM((4, 512, 1024), BF16),
            pltpu.SemaphoreType.DMA,
            pltpu.SemaphoreType.DMA,
            pltpu.SemaphoreType.DMA((3,)),
            pltpu.SemaphoreType.DMA((3,)),
            pltpu.SemaphoreType.DMA((NZ,)),
            pltpu.SemaphoreType.DMA((NZ,)),
            pltpu.SemaphoreType.DMA((NYC * NX,)),
            pltpu.SemaphoreType.DMA((NYC * NX,)),
        ],
        compiler_params=pltpu.CompilerParams(
            collective_id=0, has_side_effects=True, vmem_limit_bytes=67043328
        ),
    )(sky_rows, arc_start, arc_count, owner_modes, owner_modes.reshape(4, 128), leg_rows)
    return out.reshape(8, 2, 8, 4, 128).transpose(0, 1, 3, 2, 4).reshape(8, 2, 4, 1024)


def solution(mesh):
    return jax.shard_map(
        local,
        mesh=mesh,
        in_specs=(
            P(None, None, "blk", "lblk"),
            P(None, "blk"),
            P(None, "blk"),
            P(),
            P("blk", None, None, "lblk"),
        ),
        out_specs=P(None, None, "blk", "lblk"),
        check_vma=False,
    )
```

```python
import math

import jax
import jax.numpy as jnp
from jax import lax
from jax.experimental import pallas as pl
from jax.experimental.pallas import tpu as pltpu
from jax.sharding import PartitionSpec as P

RLEN = 16384
DIFFUSION = 0.2
NX = 4
NZ = 16
NYC = 8
NBLK = NZ * NYC
LANES = 128
G_STRIDE = 40
BF16 = jnp.bfloat16
F32 = jnp.float32


def unit_circle(t):
    t = t & (RLEN - 1)
    q = (t + 2048) >> 12
    theta = (t - (q << 12)).astype(F32) * (2.0 * math.pi / RLEN)
    u = theta * theta
    s = theta * (1.0 + u * (-1.0 / 6 + u * (1.0 / 120 + u * (-1.0 / 5040 + u * (1.0 / 362880)))))
    c = 1.0 + u * (-0.5 + u * (1.0 / 24 + u * (-1.0 / 720 + u * (1.0 / 40320))))
    odd = (q & 1) == 1
    big = jnp.where(odd, s, c)
    small = jnp.where(odd, c, s)
    cos = jnp.where(((q + 1) & 2) == 2, -big, big)
    sin = jnp.where((q & 2) == 2, -small, small)
    return cos, sin


def small_angle(theta):
    u = theta * theta
    s = theta * (1.0 + u * (-1.0 / 6 + u * (1.0 / 120 + u * (-1.0 / 5040))))
    c = 1.0 + u * (-0.5 + u * (1.0 / 24 + u * (-1.0 / 720 + u * (1.0 / 40320))))
    return c, s


def iota(shape, dim):
    return lax.broadcasted_iota(jnp.int32, shape, dim)


def kernel(
    sky_hbm,
    start_hbm,
    count_hbm,
    modes_hbm,
    leg_hbm,
    out_ref,
    start_ref,
    count_ref,
    modes_s,
    modes_v,
    sky_v,
    x_ref,
    y_ref,
    table_ref,
    turn_ref,
    modes_ref,
    rs_send,
    rs_recv,
    u_ref,
    z_send,
    z_recv,
    zf_ref,
    g_send,
    g_recv,
    gf_ref,
    leg_raw,
    leg_tmp,
    leg_prep,
    sky_sem,
    leg_sem,
    small_sem,
    rs_ssem,
    rs_rsem,
    z_ssem,
    z_rsem,
    g_ssem,
    g_rsem,
):
    blk = lax.axis_index("blk")
    col = lax.axis_index("lblk")
    my_z = blk >> 3
    my_yc = blk & 7

    barrier = pltpu.get_barrier_semaphore()

    def place(z, yc, x):
        return {"blk": ((z & 15) << 3) | (yc & 7), "lblk": x & 3}

    def greet(target):
        pl.semaphore_signal(
            barrier, inc=1, device_id=target, device_id_type=pl.DeviceIdType.MESH
        )

    small = [
        pltpu.make_async_copy(modes_hbm, modes_v, small_sem.at[0]),
        pltpu.make_async_copy(start_hbm, start_ref, small_sem.at[1]),
        pltpu.make_async_copy(count_hbm, count_ref, small_sem.at[2]),
        pltpu.make_async_copy(modes_hbm, modes_s, small_sem.at[3]),
    ]
    sky_copy = pltpu.make_async_copy(sky_hbm, sky_v, sky_sem)
    leg_copy = pltpu.make_async_copy(leg_hbm, leg_raw, leg_sem)
    for copy in small[:3]:
        copy.start()
    sky_copy.start()
    small[3].start()
    leg_copy.start()
    for dx in (2, 1, 3):
        greet(place(my_z, my_yc, col + dx))
    for dz in (8, 7, 9, 6, 10, 5, 11, 4, 12, 3, 13, 2, 14, 1, 15):
        greet(place(my_z + dz, my_yc, col))
    for dyc in range(1, 8):
        for dx in range(4):
            greet(place(my_z, my_yc + dyc, col + dx))

    small[0].wait()
    lane8 = iota((8, LANES), 1)
    pick = (4 * (lane8 & 31) + iota((8, LANES), 0)) & (LANES - 1)
    modes = jnp.zeros((8, LANES), jnp.int32)
    for r in range(4):
        row = jnp.broadcast_to(modes_v[r : r + 1, :], (8, LANES))
        got = jnp.take_along_axis(row, pick, axis=1)
        modes = jnp.where((lane8 >> 5) == r, got, modes)
    modes_ref[...] = modes

    steps = (2, 1, 3, 0)
    b_index = iota((LANES, LANES), 0)
    lt_index = iota((64, LANES), 0) >> 2
    for step, ahead in enumerate(steps):
        m_row = modes_ref[pl.ds((col + ahead) & 3, 1), :]
        for hi in range(2):
            c, sn = unit_circle((b_index + 2048 * hi) * m_row)
            table_ref[step, hi * 128 : hi * 128 + 128, 0:128] = c.astype(BF16)
            table_ref[step, hi * 128 : hi * 128 + 128, 128:256] = (-sn).astype(BF16)
        c, sn = unit_circle((col * 4096 + lt_index * LANES) * m_row)
        turn_ref[step, 0] = c * (1.0 / 128)
        turn_ref[step, 1] = sn * (-1.0 / 128)

    small[1].wait()
    small[2].wait()
    sky_copy.wait()
    sub8 = iota((8, LANES), 0)
    k8 = sub8 & 3
    for h in range(2):
        start8 = jnp.zeros((8, LANES), jnp.int32)
        count8 = jnp.zeros((8, LANES), jnp.int32)
        for k in range(4):
            start8 = jnp.where(k8 == k, start_ref[h, k], start8)
            count8 = jnp.where(k8 == k, count_ref[h, k], count8)
        base8 = col * 4096 + (sub8 >> 2) * LANES + lane8 - start8
        keep = [
            ((base8 + 256 * t) & (RLEN - 1)) < count8 for t in range(16)
        ]
        keep = [jnp.where(b, 1.0, 0.0).astype(F32) for b in keep]
        keep_lo = jnp.concatenate(keep[:8], axis=0)
        keep_hi = jnp.concatenate(keep[8:], axis=0)
        for x in range(8):
            r0 = (x * 2 + h) * 128
            lo = sky_v[pl.ds(r0, 64), :].astype(F32)
            hi = sky_v[pl.ds(r0 + 64, 64), :].astype(F32)
            x_ref[pl.ds((x * 2 + h) * 64, 64), 0:128] = (lo * keep_lo).astype(BF16)
            x_ref[pl.ds((x * 2 + h) * 64, 64), 128:256] = (hi * keep_hi).astype(BF16)

    upper = sub8 < 4
    for step, ahead in enumerate(steps):
        chunk = (col + ahead) & 3
        y_ref[step] = jnp.dot(x_ref[...], table_ref[step], preferred_element_type=F32)
        w_c = turn_ref[step, 0]
        w_s = turn_ref[step, 1]
        for x in range(8):
            acc = []
            for h in range(2):
                re = jnp.zeros((8, LANES), F32)
                im = jnp.zeros((8, LANES), F32)
                for t in range(8):
                    r0 = (x * 2 + h) * 64 + t * 8
                    yc = y_ref[step, r0 : r0 + 8, 0:128]
                    ys = y_ref[step, r0 : r0 + 8, 128:256]
                    wc = w_c[t * 8 : t * 8 + 8]
                    ws = w_s[t * 8 : t * 8 + 8]
                    re = re + (yc * wc - ys * ws)
                    im = im + (yc * ws + ys * wc)
                acc.append((re, im))
            for part in range(2):
                plus = acc[0][part] + acc[1][part]
                minus = acc[0][part] - acc[1][part]
                plus = plus + pltpu.roll(plus, 4, axis=0)
                minus = minus + pltpu.roll(minus, 4, axis=0)
                r0 = part * 64 + x * 8
                u_ref[r0 : r0 + 8, :] = jnp.where(upper, plus, minus)
        if ahead == 0:
            break
        rs_send[step] = u_ref[...].astype(BF16)
        if step == 0:
            pl.semaphore_wait(barrier, NZ - 1 + NYC * NX - 1)
        pltpu.make_async_remote_copy(
            src_ref=rs_send.at[step],
            dst_ref=rs_recv.at[step],
            send_sem=rs_ssem.at[step],
            recv_sem=rs_rsem.at[step],
            device_id={"blk": blk, "lblk": chunk},
            device_id_type=pl.DeviceIdType.MESH,
        ).start()

    def prepare(s):
        def group(gb, carry):
            raw = leg_raw[s, pl.ds(gb * 512, 512), :].astype(F32)
            for g in range(16):
                leg_tmp[g * G_STRIDE : g * G_STRIDE + 32, :] = raw[g * 32 : g * 32 + 32]
            for lt in range(8):
                for r in range(4):
                    rows = leg_tmp[pl.ds(lt * 4 + r, 16, stride=G_STRIDE), :]
                    leg_prep[s, pl.ds(r * 128 + gb * 16, 16), lt * 128 : lt * 128 + 128] = (
                        rows.astype(BF16)
                    )
            return carry

        lax.fori_loop(0, 8, group, 0)

    leg_copy.wait()
    prepare(0)

    def rs_copy(step):
        return pltpu.make_async_remote_copy(
            src_ref=rs_send.at[step],
            dst_ref=rs_recv.at[step],
            send_sem=rs_ssem.at[step],
            recv_sem=rs_rsem.at[step],
            device_id={"blk": blk, "lblk": (col + 1) & 3},
            device_id_type=pl.DeviceIdType.MESH,
        )

    total = u_ref[...]
    for step in range(3):
        rs_copy(step).wait()
    for step in range(3):
        total = total + rs_recv[step].astype(F32)
    u_ref[...] = total

    ordered = jnp.concatenate(
        [
            u_ref[pl.ds(part * 64 + sign * 4 + k, 8, stride=8), :]
            for k in range(4)
            for part in range(2)
            for sign in range(2)
        ],
        axis=0,
    )
    turned = ordered.T
    for z in range(NZ):
        z_send[z] = turned[z * 8 : z * 8 + 8].astype(BF16)

    for d in (8, 7, 9, 6, 10, 5, 11, 4, 12, 3, 13, 2, 14, 1, 15):
        pltpu.make_async_remote_copy(
            src_ref=z_send.at[(my_z + d) & 15],
            dst_ref=z_recv.at[my_z],
            send_sem=z_ssem,
            recv_sem=z_rsem,
            device_id=place(my_z + d, my_yc, col),
            device_id_type=pl.DeviceIdType.MESH,
        ).start()
    z_recv[my_z] = z_send[my_z]
    prepare(1)
    prepare(2)
    prepare(3)
    small[3].wait()
    others = pl.ds(0, NZ - 1)
    pltpu.make_async_remote_copy(
        src_ref=z_send.at[others],
        dst_ref=z_recv.at[others],
        send_sem=z_ssem,
        recv_sem=z_rsem,
        device_id=place(my_z + 1, my_yc, col),
        device_id_type=pl.DeviceIdType.MESH,
    ).wait()
    for z in range(NZ):
        zf_ref[z * 8 : z * 8 + 8, :] = z_recv[z].astype(F32)
    for yc in range(NYC):
        g_send[yc] = zf_ref[pl.ds(yc, NZ, stride=8), :].astype(BF16)

    for dx in (2, 1, 3, 0):
        for dyc in (4, 5, 3, 2, 6, 7, 1, 0):
            if dx or dyc:
                pltpu.make_async_remote_copy(
                    src_ref=g_send.at[(my_yc + dyc) & 7],
                    dst_ref=g_recv.at[col, my_yc],
                    send_sem=g_ssem.at[dx],
                    recv_sem=g_rsem.at[dx],
                    device_id=place(my_z, my_yc + dyc, col + dx),
                    device_id_type=pl.DeviceIdType.MESH,
                ).start()
    g_recv[col, my_yc] = g_send[my_yc]

    lane_row = iota((8, LANES), 1)
    degree = iota((8, 1024), 1) + col * 1024
    for dx in range(NX):
        group = pl.ds(0, NYC - 1 if dx == 0 else NYC)
        pltpu.make_async_remote_copy(
            src_ref=g_send.at[group],
            dst_ref=g_recv.at[(col - dx) & 3, group],
            send_sem=g_ssem.at[dx],
            recv_sem=g_rsem.at[dx],
            device_id=place(my_z, my_yc + 1, col),
            device_id_type=pl.DeviceIdType.MESH,
        ).wait()
    for ahead in range(NX):
        source = (col - ahead) & 3
        for yc in range(NYC):
            gf_ref[ahead, yc * NZ : yc * NZ + NZ, :] = g_recv[source, yc].astype(F32)
        by_cycle = jnp.concatenate(
            [gf_ref[ahead, pl.ds(z, NYC, stride=NZ), :] for z in range(NZ)], axis=0
        )
        turned = by_cycle.T
        mode = modes_s[blk >> 5, ((blk & 31) << 2) | source]
        theta = jnp.full((8, LANES), mode, jnp.int32).astype(F32) * (math.pi / RLEN)
        turn_c, turn_s = small_angle(theta)
        double_c, _ = small_angle(theta * 2.0)
        centre = (1.0 - 4.0 * DIFFUSION) + 2.0 * DIFFUSION * double_c
        rows = {}
        for sign in range(2):
            smooth = {}
            for part in range(2):
                a = [
                    turned[(k * 4 + part * 2 + sign) * 8 : (k * 4 + part * 2 + sign) * 8 + 8]
                    for k in range(4)
                ]
                above = jnp.where(lane_row == 0, 0.0, pltpu.roll(a[3], 1, axis=1))
                edge = a[3] if sign == 0 else -a[3]
                below = jnp.where(
                    lane_row == LANES - 1, edge, pltpu.roll(a[0], LANES - 1, axis=1)
                )
                full = [above] + a + [below]
                for k in range(4):
                    smooth[part, k] = centre * a[k] + DIFFUSION * (full[k] + full[k + 2])
            for k in range(4):
                re, im = smooth[0, k], smooth[1, k]
                if k % 2:
                    re, im = re * turn_c + im * turn_s, im * turn_c - re * turn_s
                rows[sign, 0, k] = re
                rows[sign, 1, k] = im
        lhs = jnp.concatenate(
            [
                jnp.concatenate(
                    [rows[sign, part, k] for sign in range(2) for part in range(2)], axis=0
                )
                for k in range(4)
            ],
            axis=1,
        ).astype(BF16)
        sums = jnp.dot(lhs, leg_prep[source], preferred_element_type=F32)
        even = ((degree + mode) & 1) == 0
        inside = degree >= mode
        for part in range(2):
            chosen = jnp.where(
                even, sums[part * 8 : part * 8 + 8], sums[16 + part * 8 : 24 + part * 8]
            )
            chosen = jnp.where(inside, chosen, 0.0)
            for lt in range(8):
                out_ref[pl.ds(part * 32 + lt * 4 + source, 8, stride=64), :] = chosen[
                    :, lt * 128 : lt * 128 + 128
                ]


def local(sky, arc_start, arc_count, owner_modes, legendre):
    sky_rows = sky.reshape(16, 4, 32, 128).transpose(0, 2, 1, 3).reshape(2048, 128)
    leg_rows = (
        legendre.reshape(4, 128, 4, 8, 128).transpose(0, 1, 3, 2, 4).reshape(4, 4096, 128)
    )
    operands = [sky_rows, arc_start, arc_count, owner_modes.reshape(4, 128), leg_rows]
    operands = [pltpu.with_memory_space_constraint(a, pltpu.HBM) for a in operands]
    out = pl.pallas_call(
        kernel,
        out_shape=pltpu.VMEM((512, 128), F32),
        in_specs=[pl.BlockSpec(memory_space=pltpu.HBM)] * 5,
        out_specs=pl.BlockSpec(memory_space=pltpu.VMEM),
        scratch_shapes=[
            pltpu.SMEM((2, 4), jnp.int32),
            pltpu.SMEM((2, 4), jnp.int32),
            pltpu.SMEM((4, 128), jnp.int32),
            pltpu.VMEM((4, 128), jnp.int32),
            pltpu.VMEM((2048, 128), BF16),
            pltpu.VMEM((1024, 256), BF16),
            pltpu.VMEM((4, 1024, 256), F32),
            pltpu.VMEM((4, 256, 256), BF16),
            pltpu.VMEM((4, 2, 64, 128), F32),
            pltpu.VMEM((8, 128), jnp.int32),
            pltpu.VMEM((3, 128, 128), BF16),
            pltpu.VMEM((3, 128, 128), BF16),
            pltpu.VMEM((128, 128), F32),
            pltpu.VMEM((NZ, 8, 128), BF16),
            pltpu.VMEM((NZ, 8, 128), BF16),
            pltpu.VMEM((128, 128), F32),
            pltpu.VMEM((NYC, NZ, 128), BF16),
            pltpu.VMEM((NX, NYC, NZ, 128), BF16),
            pltpu.VMEM((4, 128, 128), F32),
            pltpu.VMEM((4, 4096, 128), BF16),
            pltpu.VMEM((16 * G_STRIDE, 128), F32),
            pltpu.VMEM((4, 512, 1024), BF16),
            pltpu.SemaphoreType.DMA,
            pltpu.SemaphoreType.DMA,
            pltpu.SemaphoreType.DMA((4,)),
            pltpu.SemaphoreType.DMA((3,)),
            pltpu.SemaphoreType.DMA((3,)),
            pltpu.SemaphoreType.DMA,
            pltpu.SemaphoreType.DMA,
            pltpu.SemaphoreType.DMA((NX,)),
            pltpu.SemaphoreType.DMA((NX,)),
        ],
        compiler_params=pltpu.CompilerParams(
            collective_id=0, has_side_effects=True, vmem_limit_bytes=48 * 1024 * 1024
        ),
    )(*operands)
    return out.reshape(8, 2, 8, 4, 128).transpose(0, 1, 3, 2, 4).reshape(8, 2, 4, 1024)


def solution(mesh):
    return jax.shard_map(
        local,
        mesh=mesh,
        in_specs=(
            P(None, None, "blk", "lblk"),
            P(None, "blk"),
            P(None, "blk"),
            P(),
            P("blk", None, None, "lblk"),
        ),
        out_specs=P(None, None, "blk", "lblk"),
        check_vma=False,
    )
```
